16 devices in a mesh: fsdp: 2 (over z), ep: 8 (over y, x, core).
Axes of the slice: x: 2, y: 2, z: 2, core: 2. Of those that a mesh axis runs over, the one named last changes fastest.
Arguments:
- x_tok: bfloat16 [32768, 1024], P(('ep', 'fsdp'))
- dy_tok: bfloat16 [32768, 1024], P(('ep', 'fsdp'))
- expert_ids: int32 [32768, 8], P(('ep', 'fsdp'))
- expert_slot: int32 [32768, 8], P(('ep', 'fsdp'))
- w_router: bfloat16 [1024, 32], replicated
- w_gate: bfloat16 [32, 1024, 512], P('ep', 'fsdp')
- w_up: bfloat16 [32, 1024, 512], P('ep', 'fsdp')
- w_down: bfloat16 [32, 512, 1024], P('ep', None, 'fsdp')
Outputs:
- output 1: bfloat16 [32768, 1024], P(('ep', 'fsdp'))
- output 2: float32 [], replicated
- output 3: bfloat16 [32768, 1024], P(('ep', 'fsdp'))
- output 4: float32 [1024, 32], replicated
- output 5: bfloat16 [32, 1024, 512], P('ep', 'fsdp')
- output 6: bfloat16 [32, 1024, 512], P('ep', 'fsdp')
- output 7: bfloat16 [32, 512, 1024], P('ep', None, 'fsdp')
All inputs are finite; a program needn't handle non-finite values.
Results may differ from the reference program's by a relative error of at most 0.0106918.
Values are sent between devices in bfloat16 or wider.
A program may use at most 1 GiB of HBM per device.

```python
import jax
import jax.numpy as jnp
from jax import lax

D_MODEL = 1024
D_FF = 512
EXPERTS = 32
TOP_K = 8
TOK_DEV = 2048
GROUPS = 16
TOKENS = TOK_DEV * GROUPS
CAPACITY = 5 * TOK_DEV * TOP_K // (4 * EXPERTS)
AUX_COEF = 0.01


def draw_routing(key):
    key_hot, key_spread, key_noise = jax.random.split(key, 3)
    hot_count = max(1, TOP_K // 2)
    hot_bias = min(30, 200 * TOP_K // EXPERTS)
    hot_score = jax.random.randint(key_hot, (EXPERTS,), 0, 1000) * EXPERTS + jnp.arange(EXPERTS)
    hot_ids = lax.top_k(hot_score, hot_count)[1]
    is_hot = jnp.any(hot_ids[:, None] == jnp.arange(EXPERTS)[None, :], axis=0)
    bias = jnp.where(is_hot, hot_bias, 0) + jax.random.randint(key_spread, (EXPERTS,), 0, 8)
    noise = jax.random.randint(key_noise, (TOKENS, EXPERTS), 0, 100)
    score = (noise + bias[None, :]) * EXPERTS + jnp.arange(EXPERTS)[None, :]
    expert_ids = lax.top_k(score, TOP_K)[1].astype(jnp.int32)
    grouped = expert_ids.reshape(GROUPS, TOK_DEV * TOP_K)

    def group_slots(ids_row):
        onehot = (ids_row[:, None] == jnp.arange(EXPERTS)[None, :]).astype(jnp.int32)
        before = jnp.cumsum(onehot, axis=0) - onehot
        position = jnp.sum(before * onehot, axis=1)
        return jnp.where(position < CAPACITY, position, -1)

    expert_slot = lax.map(group_slots, grouped).reshape(TOKENS, TOP_K).astype(jnp.int32)
    return expert_ids, expert_slot


def setup_inputs(seed: int = 0) -> dict:
    keys = jax.random.split(jax.random.key(seed), 7)
    x_tok = jax.random.normal(keys[0], (TOKENS, D_MODEL), jnp.float32).astype(jnp.bfloat16)
    dy_tok = (jax.random.normal(keys[1], (TOKENS, D_MODEL), jnp.float32) * D_MODEL ** -0.5).astype(jnp.bfloat16)
    expert_ids, expert_slot = draw_routing(keys[2])
    w_router = (jax.random.normal(keys[3], (D_MODEL, EXPERTS), jnp.float32) * 2.0 * D_MODEL ** -0.5).astype(jnp.bfloat16)
    w_gate = (jax.random.normal(keys[4], (EXPERTS, D_MODEL, D_FF), jnp.float32) * D_MODEL ** -0.5).astype(jnp.bfloat16)
    w_up = (jax.random.normal(keys[5], (EXPERTS, D_MODEL, D_FF), jnp.float32) * D_MODEL ** -0.5).astype(jnp.bfloat16)
    w_down = (jax.random.normal(keys[6], (EXPERTS, D_FF, D_MODEL), jnp.float32) * D_FF ** -0.5).astype(jnp.bfloat16)
    return {'x_tok': x_tok, 'dy_tok': dy_tok, 'expert_ids': expert_ids, 'expert_slot': expert_slot,
            'w_router': w_router, 'w_gate': w_gate, 'w_up': w_up, 'w_down': w_down}


def reference(x_tok, dy_tok, expert_ids, expert_slot, w_router, w_gate, w_up, w_down):
    gate_f32 = w_gate.astype(jnp.float32)
    up_f32 = w_up.astype(jnp.float32)
    down_f32 = w_down.astype(jnp.float32)
    n_slots = EXPERTS * CAPACITY
    logits = jnp.dot(x_tok, w_router, preferred_element_type=jnp.float32)
    prob_all = jax.nn.softmax(logits, axis=-1)
    gate = jnp.take_along_axis(prob_all, expert_ids, axis=1)
    counts = jax.ops.segment_sum(jnp.ones((TOKENS * TOP_K,), jnp.float32), expert_ids.reshape(-1), num_segments=EXPERTS)
    load_frac = counts / (TOKENS * TOP_K)
    aux_loss = AUX_COEF * EXPERTS * jnp.sum(load_frac * jnp.mean(prob_all, axis=0))
    pair_ids = jnp.arange(1, TOK_DEV * TOP_K + 1, dtype=jnp.int32)

    def group_pass(carry, group):
        acc_gate, acc_up, acc_down = carry
        x_grp, dy_grp, ids_grp, slot_grp, gate_grp = group
        flat_ids = ids_grp.reshape(-1)
        flat_slot = slot_grp.reshape(-1)
        dest_row = jnp.where(flat_slot >= 0, flat_ids * CAPACITY + flat_slot, n_slots)
        pair_src = jax.ops.segment_sum(pair_ids, dest_row, num_segments=n_slots)
        filled = pair_src > 0
        pair_pos = jnp.where(filled, pair_src - 1, 0)
        tok_pos = jnp.where(filled, pair_pos // TOP_K, TOK_DEV)
        in_buf = jnp.take(x_grp, tok_pos, axis=0, mode='fill', fill_value=0).reshape(EXPERTS, CAPACITY, D_MODEL).astype(jnp.float32)
        h_gate = jnp.einsum('ecd,edf->ecf', in_buf, gate_f32)
        h_up = jnp.einsum('ecd,edf->ecf', in_buf, up_f32)
        sig_gate = jax.nn.sigmoid(h_gate)
        act_buf = (h_gate * sig_gate * h_up).astype(jnp.bfloat16).astype(jnp.float32)
        out_buf = jnp.einsum('ecf,efd->ecd', act_buf, down_f32).astype(jnp.bfloat16)
        pair_out = jnp.take(out_buf.reshape(n_slots, D_MODEL), dest_row, axis=0, mode='fill', fill_value=0).reshape(TOK_DEV, TOP_K, D_MODEL).astype(jnp.float32)
        y_grp = jnp.sum(gate_grp[:, :, None] * pair_out, axis=1).astype(jnp.bfloat16)
        d_gate = jnp.einsum('td,tjd->tj', dy_grp.astype(jnp.float32), pair_out)
        gate_slot = jnp.where(filled, jnp.take(gate_grp.reshape(-1), pair_pos), 0.0)
        dy_slot = jnp.take(dy_grp, tok_pos, axis=0, mode='fill', fill_value=0).astype(jnp.float32)
        d_out = (gate_slot[:, None] * dy_slot).astype(jnp.bfloat16).astype(jnp.float32).reshape(EXPERTS, CAPACITY, D_MODEL)
        d_act = jnp.einsum('ecd,efd->ecf', d_out, down_f32).astype(jnp.bfloat16).astype(jnp.float32)
        d_hgate = (d_act * h_up * sig_gate * (1.0 + h_gate * (1.0 - sig_gate))).astype(jnp.bfloat16).astype(jnp.float32)
        d_hup = (d_act * h_gate * sig_gate).astype(jnp.bfloat16).astype(jnp.float32)
        d_in = (jnp.einsum('ecf,edf->ecd', d_hgate, gate_f32) + jnp.einsum('ecf,edf->ecd', d_hup, up_f32)).astype(jnp.bfloat16)
        acc_gate = acc_gate + jnp.einsum('ecd,ecf->edf', in_buf, d_hgate)
        acc_up = acc_up + jnp.einsum('ecd,ecf->edf', in_buf, d_hup)
        acc_down = acc_down + jnp.einsum('ecf,ecd->efd', act_buf, d_out)
        pair_dx = jnp.take(d_in.reshape(n_slots, D_MODEL), dest_row, axis=0, mode='fill', fill_value=0).reshape(TOK_DEV, TOP_K, D_MODEL)
        dx_grp = jnp.sum(pair_dx.astype(jnp.float32), axis=1)
        return (acc_gate, acc_up, acc_down), (y_grp, d_gate, dx_grp)

    init = (jnp.zeros((EXPERTS, D_MODEL, D_FF), jnp.float32), jnp.zeros((EXPERTS, D_MODEL, D_FF), jnp.float32),
            jnp.zeros((EXPERTS, D_FF, D_MODEL), jnp.float32))
    grouped = (x_tok.reshape(GROUPS, TOK_DEV, D_MODEL), dy_tok.reshape(GROUPS, TOK_DEV, D_MODEL),
               expert_ids.reshape(GROUPS, TOK_DEV, TOP_K), expert_slot.reshape(GROUPS, TOK_DEV, TOP_K),
               gate.reshape(GROUPS, TOK_DEV, TOP_K))
    sums, per_group = lax.scan(group_pass, init, grouped)
    y_grp, d_gate, dx_exp = per_group
    y_out = y_grp.reshape(TOKENS, D_MODEL)
    d_gate = d_gate.reshape(TOKENS, TOP_K)
    dx_exp = dx_exp.reshape(TOKENS, D_MODEL)
    match = expert_ids[:, :, None] == jnp.arange(EXPERTS)[None, None, :]
    d_prob = jnp.sum(jnp.where(match, d_gate[:, :, None], 0.0), axis=1) + AUX_COEF * EXPERTS * load_frac[None, :]
    d_logit = prob_all * (d_prob - jnp.sum(prob_all * d_prob, axis=-1, keepdims=True))
    d_logit_b = d_logit.astype(jnp.bfloat16)
    dx_tok = (dx_exp + jnp.dot(d_logit_b, w_router.T, preferred_element_type=jnp.float32)).astype(jnp.bfloat16)
    dw_router = jnp.dot(x_tok.T, d_logit_b, preferred_element_type=jnp.float32)
    acc_gate, acc_up, acc_down = sums
    return (y_out, aux_loss, dx_tok, dw_router, acc_gate.astype(jnp.bfloat16), acc_up.astype(jnp.bfloat16),
            acc_down.astype(jnp.bfloat16))
```

```python
import functools

import jax
import jax.numpy as jnp
from jax import lax
from jax.experimental import pallas as pl
from jax.experimental.pallas import tpu as pltpu
from jax.sharding import PartitionSpec as P


AUX_COEF = 0.01
BLK = 1024
TILE = 256
X, Y = 2, 4
KERNEL_FLOPS = 100_000_000
F32 = jnp.float32
BF16 = jnp.bfloat16


def dot(a, b, ca, cb):
    return lax.dot_general(a, b, (((ca,), (cb,)), ((), ())), preferred_element_type=F32)


def expert_kernel(has_init, nt_ref, xd0_ref, xd1_ref, pos_ref, gate_ref, wg_ref, wu_ref, wd_ref, *rest):
    if has_init:
        ig_ref, iu_ref, id_ref = rest[:3]
        rest = rest[3:]
    (yd0_ref, yd1_ref, dgate_ref, og_ref, ou_ref, od_ref,
     xd_ref, yd_ref, ag_ref, au_ref, ad_ref, tok_sem, in_sem, out_sem) = rest
    b = pl.program_id(0)
    e = pl.program_id(1)
    last = pl.num_programs(0) - 1
    n_exp = og_ref.shape[0]
    d_model = xd_ref.shape[3]
    tok_in = [pltpu.make_async_copy(src, xd_ref.at[k], tok_sem.at[k]) for k, src in enumerate((xd0_ref, xd1_ref))]
    tok_out = [pltpu.make_async_copy(yd_ref.at[k], dst, tok_sem.at[2 + k]) for k, dst in enumerate((yd0_ref, yd1_ref))]

    def in_copies(k):
        return [pltpu.make_async_copy(src.at[k], dst.at[k], in_sem.at[k, i])
                for i, (src, dst) in enumerate(((ig_ref, ag_ref), (iu_ref, au_ref), (id_ref, ad_ref)))]

    def out_copies(k):
        return [pltpu.make_async_copy(src.at[k], dst.at[k], out_sem.at[k, i])
                for i, (src, dst) in enumerate(((ag_ref, og_ref), (au_ref, ou_ref), (ad_ref, od_ref)))]

    @pl.when((b == 0) & (e == 0))
    def _():
        tok_in[0].start()
        if has_init:
            for c in in_copies(0):
                c.start()
        tok_in[1].start()
        if has_init:
            for k in range(1, n_exp):
                for c in in_copies(k):
                    c.start()

    for k in range(2):
        @pl.when((b == k) & (e == 0))
        def _():
            tok_in[k].wait()

    @pl.when(e == 0)
    def _():
        yd_ref[b] = jnp.zeros(yd_ref.shape[1:], F32)

    @pl.when(b == 0)
    def _():
        if has_init:
            for c in in_copies(e):
                c.wait()
        else:
            ag_ref[e] = jnp.zeros(ag_ref.shape[1:], F32)
            au_ref[e] = jnp.zeros(au_ref.shape[1:], F32)
            ad_ref[e] = jnp.zeros(ad_ref.shape[1:], F32)

    dgate_ref[...] = jnp.zeros(dgate_ref.shape, F32)
    gate_row = gate_ref[0, 0]

    def tile(i, carry):
        pos = pos_ref[0, 0]
        rows = (lax.broadcasted_iota(jnp.int32, (TILE, BLK), 0) + i * TILE).astype(F32)
        hit = rows == pos
        pick = jnp.where(hit, 1.0, 0.0).astype(BF16)
        gate_c = jnp.sum(jnp.where(hit, gate_row, 0.0), axis=1, keepdims=True)
        xc = dot(pick, xd_ref[b, 0], 1, 0).astype(BF16)
        dyc = dot(pick, xd_ref[b, 1], 1, 0)
        hg = dot(xc, wg_ref[0], 1, 0)
        hu = dot(xc, wu_ref[0], 1, 0)
        sig = jax.nn.sigmoid(hg)
        act = (hg * sig * hu).astype(BF16)
        do = (gate_c * dyc).astype(BF16)
        da = dot(do, wd_ref[0], 1, 1).astype(BF16).astype(F32)
        dhg = (da * hu * sig * (1.0 + hg * (1.0 - sig))).astype(BF16)
        dhu = (da * hg * sig).astype(BF16)
        o = dot(act, wd_ref[0], 1, 0).astype(BF16)
        dgate_c = jnp.sum(dyc * o.astype(F32), axis=1, keepdims=True)
        dgate_ref[0, 0] += jnp.sum(jnp.where(hit, dgate_c, 0.0), axis=0, keepdims=True)
        db = (dot(dhg, wg_ref[0], 1, 1) + dot(dhu, wu_ref[0], 1, 1)).astype(BF16)
        ag_ref[e] += dot(xc, dhg, 0, 0)
        au_ref[e] += dot(xc, dhu, 0, 0)
        ad_ref[e] += dot(act, do, 0, 0)
        gate_t = jnp.transpose(jnp.broadcast_to(gate_row, (8, BLK)))[:, :1]
        width = 256
        for c in range(d_model // width):
            cols = slice(c * width, (c + 1) * width)
            yd_ref[b, 0, :, cols] += gate_t * dot(pick, o[:, cols], 0, 0)
            yd_ref[b, 1, :, cols] += dot(pick, db[:, cols], 0, 0)
        return carry

    lax.fori_loop(0, nt_ref[b, e], tile, 0)

    for k in range(2):
        @pl.when((b == k) & (e == n_exp - 1))
        def _():
            tok_out[k].start()

    @pl.when(b == last)
    def _():
        for c in out_copies(e):
            c.start()

        @pl.when(e == n_exp - 1)
        def _():
            for k in range(2):
                tok_out[k].wait()
            for k in range(n_exp):
                for c in out_copies(k):
                    c.wait()


def experts(nt, xd0, xd1, pos, gate, wg, wu, wd, init):
    n_exp, d_model, d_ff = wg.shape
    row = pl.BlockSpec((1, 1, 1, BLK), lambda b, e, nt: (b, e, 0, 0))
    up = pl.BlockSpec((1, d_model, d_ff), lambda b, e, nt: (e, 0, 0))
    down = pl.BlockSpec((1, d_ff, d_model), lambda b, e, nt: (e, 0, 0))
    hbm = pl.BlockSpec(memory_space=pl.ANY)
    acc_up = jax.ShapeDtypeStruct((n_exp, d_model, d_ff), F32)
    acc_down = jax.ShapeDtypeStruct((n_exp, d_ff, d_model), F32)
    out_tok = jax.ShapeDtypeStruct((2, BLK, d_model), F32)
    return pl.pallas_call(
        functools.partial(expert_kernel, init is not None),
        grid_spec=pltpu.PrefetchScalarGridSpec(
            num_scalar_prefetch=1,
            grid=(2, n_exp),
            in_specs=[hbm, hbm, row, row, up, up, down] + ([hbm] * 3 if init is not None else []),
            out_specs=[hbm, hbm, row, hbm, hbm, hbm],
            scratch_shapes=[
                pltpu.VMEM((2, 2, BLK, d_model), BF16),
                pltpu.VMEM((2, 2, BLK, d_model), F32),
                pltpu.VMEM((n_exp, d_model, d_ff), F32),
                pltpu.VMEM((n_exp, d_model, d_ff), F32),
                pltpu.VMEM((n_exp, d_ff, d_model), F32),
                pltpu.SemaphoreType.DMA((4,)),
                pltpu.SemaphoreType.DMA((n_exp, 3)),
                pltpu.SemaphoreType.DMA((n_exp, 3)),
            ],
        ),
        out_shape=[out_tok, out_tok, jax.ShapeDtypeStruct((2, n_exp, 1, BLK), F32), acc_up, acc_up, acc_down],
        input_output_aliases={8: 3, 9: 4, 10: 5} if init is not None else {},
        compiler_params=pltpu.CompilerParams(
            dimension_semantics=("arbitrary", "arbitrary"), vmem_limit_bytes=67_000_000),
        cost_estimate=pl.CostEstimate(flops=KERNEL_FLOPS, bytes_accessed=80_000_000, transcendentals=1_000_000),
    )(nt, xd0, xd1, pos, gate, wg, wu, wd, *(init or ()))


def whole(mine, axis, f_idx):
    other = lax.ppermute(mine, 'fsdp', [(0, 1), (1, 0)])
    return jnp.where(f_idx == 0, jnp.concatenate([mine, other], axis), jnp.concatenate([other, mine], axis))


def swap_halves(part, axis, f_idx):
    size = part.shape[axis] // 2
    mine = lax.dynamic_slice_in_dim(part, f_idx * size, size, axis)
    theirs = lax.dynamic_slice_in_dim(part, (1 - f_idx) * size, size, axis)
    other = lax.ppermute(theirs, 'fsdp', [(0, 1), (1, 0)])
    return (mine + other).astype(BF16)


def by_distance(a, bits):
    rest = a.shape[1:]
    a = a.reshape(2, 2, 2, *rest)
    for axis, bit in enumerate(bits):
        a = jnp.where(bit, jnp.flip(a, axis), a)
    return a.reshape(8, *rest)


def hop(a, bit):
    return lax.ppermute(a, 'ep', [(i, i ^ bit) for i in range(8)])


def solution(mesh):
    n_fsdp = mesh.shape['fsdp']
    n_ep = mesh.shape['ep']
    n_dev = n_fsdp * n_ep
    all_axes = ('fsdp', 'ep')
    tok_spec = P(('ep', 'fsdp'), None)
    up_spec = P('ep', 'fsdp', None)
    down_spec = P('ep', None, 'fsdp')

    def local_step(x_loc, dy_loc, ids_loc, slot_loc, w_router, wg_loc, wu_loc, wd_loc):
        tok_dev, _ = x_loc.shape
        top_k = ids_loc.shape[1]
        n_exp = w_router.shape[1]
        local_exp = n_exp // n_ep
        tokens = tok_dev * n_dev
        halves = tok_dev // BLK
        f_idx = lax.axis_index('fsdp')

        logits = dot(w_router, x_loc, 0, 1)
        prob = jax.nn.softmax(logits, axis=0)
        expert = jnp.arange(n_exp, dtype=jnp.int32)[None, :, None]
        match = ids_loc.T[:, None, :] == expert
        chosen = jnp.any(match, axis=0)
        kept = jnp.any(match & (slot_loc.T[:, None, :] >= 0), axis=0)
        stat = jnp.stack([jnp.sum(chosen.astype(F32), axis=1), jnp.sum(prob, axis=1)])
        stat = lax.psum(stat, all_axes)
        load_frac = stat[0] / (tokens * top_k)
        aux_loss = AUX_COEF * n_exp * jnp.sum(load_frac * stat[1] / tokens)

        upto = jnp.arange(BLK)[:, None] <= jnp.arange(BLK)[None, :]
        kept_b = kept.astype(BF16).reshape(n_exp * halves, BLK)
        place = dot(kept_b, upto.astype(BF16), 1, 0).reshape(n_exp, tok_dev) - 1.0
        pos = jnp.where(kept, place, -1.0)
        gate = jnp.where(kept, prob, 0.0)
        meta = jnp.stack([pos, gate], axis=1).reshape(n_ep, local_exp, 2, tok_dev)
        meta = lax.all_to_all(meta, 'ep', 0, 0, tiled=True)
        ep_idx = lax.axis_index('ep')
        bits = [(ep_idx // d) % 2 == 1 for d in (4, 2, 1)]
        meta = by_distance(meta, bits)
        meta = meta.reshape(n_ep, local_exp, 2, halves, BLK).transpose(3, 0, 1, 2, 4)
        pos_b = meta[:, :, :, 0:1]
        gate_b = meta[:, :, :, 1:2]
        nt = ((jnp.max(pos_b[..., 0, :], axis=-1) + TILE) / TILE).astype(jnp.int32)

        xd = {(0, h): jnp.stack([x_loc[h * BLK:(h + 1) * BLK], dy_loc[h * BLK:(h + 1) * BLK]]) for h in range(2)}
        xd[X, 0] = hop(xd[0, 0], X)
        xd[Y, 1] = hop(xd[0, 1], Y)
        xd[X, 1] = hop(xd[0, 1], X)
        xd[Y, 0] = hop(xd[0, 0], Y)
        xd[X + Y, 1] = hop(xd[Y, 1], X)
        xd[X + Y, 0] = hop(xd[X, 0], Y)
        wg, wu, wd = (whole(w, axis, f_idx) for w, axis in ((wg_loc, 1), (wu_loc, 1), (wd_loc, 2)))

        acc = None
        part, dgate, sent = {}, {}, {}
        order = ((X, 0), (Y, 1), (0, 0), (0, 1), (X + Y, 0), (X + Y, 1), (Y, 0), (X, 1))
        for k, h in order[:4]:
            xd[k + 1, h] = hop(xd[k, h], 1)
        for n, (k, h) in enumerate(order):
            nt_k = nt[h, k:k + 2]
            if n >= 2:
                nt_k, done = lax.optimization_barrier((nt_k, sent[order[n - 2]]))
                part[order[n - 2]] = done
            yd0, yd1, dgate[k, h], *acc = experts(
                nt_k, xd[k, h], xd[k + 1, h], pos_b[h, k:k + 2], gate_b[h, k:k + 2], wg, wu, wd, acc)
            other = hop(yd1, 1)
            sent[k, h] = [yd0[i] + other[i] for i in range(2)]
            if n == 2:
                for late in order[4:]:
                    xd[late], dgate[k, h] = lax.optimization_barrier((xd[late], dgate[k, h]))
                    xd[late[0] + 1, late[1]] = hop(xd[late], 1)
        for last in order[-2:]:
            part[last] = sent[last]
        direct = [[hop(part[X, 0][i], X), hop(part[Y, 1][i], Y)] for i in range(2)]
        relay = [[hop(part[X + Y, 0][i], X), hop(part[X + Y, 1][i], Y)] for i in range(2)]
        relay = [[hop(part[Y, 0][i] + relay[i][0], Y), hop(part[X, 1][i] + relay[i][1], X)]
                 for i in range(2)]
        total = [[part[0, h][i] + direct[i][h] + relay[i][h] for h in range(2)] for i in range(2)]
        y = jnp.concatenate(total[0], axis=0).astype(BF16)
        dx_exp = jnp.concatenate(total[1], axis=0)
        dgate = jnp.stack([jnp.concatenate([dgate[k, h] for k in (0, X, Y, X + Y)], axis=0) for h in range(2)], axis=3)
        dgate = by_distance(dgate.reshape(n_ep, local_exp, tok_dev), bits)
        dgate = lax.all_to_all(dgate, 'ep', 0, 0, tiled=True).reshape(n_exp, tok_dev)
        d_prob = dgate + AUX_COEF * n_exp * load_frac[:, None]
        d_logit = (prob * (d_prob - jnp.sum(prob * d_prob, axis=0, keepdims=True))).astype(BF16)
        dx = (dx_exp + dot(d_logit, w_router, 0, 1)).astype(BF16)
        dw_router = lax.psum(dot(x_loc, d_logit, 0, 1), all_axes)
        dwg, dwu, dwd = acc
        return (y, aux_loss, dx, dw_router, swap_halves(dwg, 1, f_idx), swap_halves(dwu, 1, f_idx),
                swap_halves(dwd, 2, f_idx))

    return jax.shard_map(local_step, mesh=mesh,
                         in_specs=(tok_spec, tok_spec, tok_spec, tok_spec, P(), up_spec, up_spec, down_spec),
                         out_specs=(tok_spec, P(), tok_spec, P(), up_spec, up_spec, down_spec),
                         check_vma=False)
```

```python
import functools

import jax
import jax.numpy as jnp
from jax import lax
from jax.experimental import pallas as pl
from jax.experimental.pallas import tpu as pltpu
from jax.sharding import PartitionSpec as P


AUX_COEF = 0.01
BLK = 1024
TILE = 256
X, Y = 2, 4
F32 = jnp.float32
BF16 = jnp.bfloat16


def dot(a, b, ca, cb):
    return lax.dot_general(a, b, (((ca,), (cb,)), ((), ())), preferred_element_type=F32)


def expert_kernel(n_blk, n_exp, fresh, nt_ref, pos_ref, gate_ref, wg0_ref, wg1_ref, wu0_ref, wu1_ref, wd0_ref, wd1_ref, *rest):
    n_pair = n_exp // 2
    rest = list(rest)
    take = lambda n: [rest.pop(0) for _ in range(n)]
    tok_in_refs = take(n_blk)
    acc_in_refs = [None if fresh[p] else take(2) for p in range(n_pair)]
    tok_out_refs = take(n_blk)
    dgate_ref, = take(1)
    acc_out_refs = [take(2) for _ in range(n_pair)]
    xd_ref, yd_ref, acc_ref, in_sem, out_sem, acc_in_sem, acc_out_sem = rest
    b = pl.program_id(0)
    e = pl.program_id(1)
    half = xd_ref.shape[3] // 2
    tok_in = [pltpu.make_async_copy(src, xd_ref.at[k % 2], in_sem.at[k]) for k, src in enumerate(tok_in_refs)]
    tok_out = [pltpu.make_async_copy(yd_ref.at[k % 2], dst, out_sem.at[k]) for k, dst in enumerate(tok_out_refs)]

    def acc_in(k):
        return [pltpu.make_async_copy(acc_in_refs[k // 2][s].at[k % 2], acc_ref.at[k, s], acc_in_sem.at[k, s]) for s in range(2)]

    def acc_out(k):
        return [pltpu.make_async_copy(acc_ref.at[k, s], acc_out_refs[k // 2][s].at[k % 2], acc_out_sem.at[k, s]) for s in range(2)]

    @pl.when((b == 0) & (e == 0))
    def _():
        tok_in[0].start()
        if not fresh[0]:
            for c in acc_in(0):
                c.start()

    for k in range(n_exp):
        @pl.when((b == 0) & (e == k))
        def _():
            if k + 1 < n_exp and not fresh[(k + 1) // 2]:
                for c in acc_in(k + 1):
                    c.start()
            if k == n_exp // 2 - 1:
                tok_in[1].start()

    for k in range(n_blk):
        @pl.when((b == k) & (e == 0))
        def _():
            tok_in[k].wait()
            if 1 <= k < n_blk - 1:
                tok_in[k + 1].start()
            if k >= 2:
                tok_out[k - 2].wait()

    slot = b % 2

    @pl.when(e == 0)
    def _():
        yd_ref[slot] = jnp.zeros(yd_ref.shape[1:], F32)

    def acc_ready():
        for k in range(n_exp):
            @pl.when((b == 0) & (e == k))
            def _():
                if fresh[k // 2]:
                    acc_ref[k] = jnp.zeros(acc_ref.shape[1:], F32)
                else:
                    for c in acc_in(k):
                        c.wait()

    dgate_ref[...] = jnp.zeros(dgate_ref.shape, F32)
    wg, wu, wd = (wg0_ref, wg1_ref), (wu0_ref, wu1_ref), (wd0_ref, wd1_ref)
    cols = (slice(0, half), slice(half, 2 * half))

    gate_row = gate_ref[0, 0]

    def tile(base, size, first):
        pos = pos_ref[0, 0]
        rows = (lax.broadcasted_iota(jnp.int32, (size, BLK), 0) + base).astype(F32)
        hit = rows == pos
        pick = jnp.where(hit, 1.0, 0.0).astype(BF16)
        gate_c = jnp.sum(jnp.where(hit, gate_row, 0.0), axis=1, keepdims=True)
        xc = [dot(pick, xd_ref[slot, 0, :, c], 1, 0).astype(BF16) for c in cols]
        dyc = [dot(pick, xd_ref[slot, 1, :, c], 1, 0) for c in cols]
        hg = dot(xc[0], wg[0][0], 1, 0) + dot(xc[1], wg[1][0], 1, 0)
        hu = dot(xc[0], wu[0][0], 1, 0) + dot(xc[1], wu[1][0], 1, 0)
        sig = jax.nn.sigmoid(hg)
        act = (hg * sig * hu).astype(BF16)
        do = [(gate_c * d).astype(BF16) for d in dyc]
        da = (dot(do[0], wd[0][0], 1, 1) + dot(do[1], wd[1][0], 1, 1)).astype(BF16).astype(F32)
        dhg = (da * hu * sig * (1.0 + hg * (1.0 - sig))).astype(BF16)
        dhu = (da * hg * sig).astype(BF16)
        o = [dot(act, w[0], 1, 0).astype(BF16) for w in wd]
        dgate_c = sum(jnp.sum(dyc[s] * o[s].astype(F32), axis=1, keepdims=True) for s in range(2))
        dgate_ref[0, 0] += jnp.sum(jnp.where(hit, dgate_c, 0.0), axis=0, keepdims=True)
        db = [(dot(dhg, wg[s][0], 1, 1) + dot(dhu, wu[s][0], 1, 1)).astype(BF16) for s in range(2)]
        pl.when(first)(acc_ready)
        for s in range(2):
            acc_ref[e, s, 0] += dot(xc[s], dhg, 0, 0)
            acc_ref[e, s, 1] += dot(xc[s], dhu, 0, 0)
            acc_ref[e, s, 2] += dot(act, do[s], 0, 0)
        gate_t = jnp.transpose(jnp.broadcast_to(gate_row, (8, BLK)))[:, :1]
        width = 256
        for s in range(2):
            for c in range(half // width):
                part = slice(c * width, (c + 1) * width)
                out = slice(s * half + c * width, s * half + (c + 1) * width)
                yd_ref[slot, 0, :, out] += gate_t * dot(pick, o[s][:, part], 0, 0)
                yd_ref[slot, 1, :, out] += dot(pick, db[s][:, part], 0, 0)

    def full_tile(i, carry):
        tile(i * TILE, TILE, i == 0)
        return carry

    tiles = nt_ref[b, e]
    full = jnp.right_shift(tiles, 1)
    lax.fori_loop(0, full, full_tile, 0)
    pl.when((tiles & 1) == 1)(lambda: tile(full * TILE, TILE // 2, full == 0))
    pl.when(tiles == 0)(acc_ready)

    for k in range(n_blk):
        @pl.when((b == k) & (e == n_exp - 1))
        def _():
            tok_out[k].start()

    for k in range(n_exp):
        @pl.when((b == n_blk - 1) & (e == k))
        def _():
            for c in acc_out(k):
                c.start()

    @pl.when((b == n_blk - 1) & (e == n_exp - 1))
    def _():
        for k in range(max(0, n_blk - 2), n_blk):
            tok_out[k].wait()
        for k in range(n_exp):
            for c in acc_out(k):
                c.wait()


def experts(nt, pos, gate, toks, weights, e0, acc):
    n_blk, n_exp = nt.shape
    d_model = toks[0].shape[2]
    half, d_ff = weights[0].shape[1:]
    row = pl.BlockSpec((1, 1, 1, BLK), lambda b, e, nt: (b, e, 0, 0))
    up = pl.BlockSpec((1, half, d_ff), lambda b, e, nt: (e + e0, 0, 0))
    down = pl.BlockSpec((1, d_ff, half), lambda b, e, nt: (e + e0, 0, 0))
    hbm = pl.BlockSpec(memory_space=pl.ANY)
    fresh = tuple(a is None for a in acc)
    acc_args = [r for a in acc if a is not None for r in a]
    acc_shape = jax.ShapeDtypeStruct((2, 3, half, d_ff), F32)
    first_in = 1 + 8 + n_blk
    first_out = n_blk + 1
    aliases = {}
    for p, a in enumerate(acc):
        if a is not None:
            for s in range(2):
                aliases[first_in] = first_out + 2 * p + s
                first_in += 1
    res = pl.pallas_call(
        functools.partial(expert_kernel, n_blk, n_exp, fresh),
        grid_spec=pltpu.PrefetchScalarGridSpec(
            num_scalar_prefetch=1,
            grid=(n_blk, n_exp),
            in_specs=[row, row, up, up, up, up, down, down] + [hbm] * (n_blk + len(acc_args)),
            out_specs=[hbm] * n_blk + [row] + [hbm] * (2 * len(acc)),
            scratch_shapes=[
                pltpu.VMEM((2, 2, BLK, d_model), BF16),
                pltpu.VMEM((2, 2, BLK, d_model), F32),
                pltpu.VMEM((n_exp, 2, 3, half, d_ff), F32),
                pltpu.SemaphoreType.DMA((n_blk,)),
                pltpu.SemaphoreType.DMA((n_blk,)),
                pltpu.SemaphoreType.DMA((n_exp, 2)),
                pltpu.SemaphoreType.DMA((n_exp, 2)),
            ],
        ),
        out_shape=[jax.ShapeDtypeStruct((2, BLK, d_model), F32)] * n_blk
        + [jax.ShapeDtypeStruct((n_blk, n_exp, 1, BLK), F32)] + [acc_shape] * (2 * len(acc)),
        input_output_aliases=aliases,
        compiler_params=pltpu.CompilerParams(
            dimension_semantics=("arbitrary", "arbitrary"), vmem_limit_bytes=67_000_000),
        cost_estimate=pl.CostEstimate(flops=100_000_000, bytes_accessed=80_000_000, transcendentals=1_000_000),
    )(nt, pos, gate, *weights, *toks, *acc_args)
    toks_out, dgate, acc = res[:n_blk], res[n_blk], res[n_blk + 1:]
    return toks_out, dgate, [acc[2 * p:2 * p + 2] for p in range(len(acc) // 2)]


def by_distance(a, bits):
    rest = a.shape[1:]
    a = a.reshape(2, 2, 2, *rest)
    for axis, bit in enumerate(bits):
        a = jnp.where(bit, jnp.flip(a, axis), a)
    return a.reshape(8, *rest)


def hop(a, bit):
    return lax.ppermute(a, 'ep', [(i, i ^ bit) for i in range(8)])


def hop_z(a):
    return lax.ppermute(a, 'fsdp', [(0, 1), (1, 0)])


def turn(a, f_idx):
    half = a.shape[-1] // 2
    return jnp.where(f_idx == 1, jnp.concatenate([a[..., half:], a[..., :half]], axis=-1), a)


def solution(mesh):
    n_fsdp = mesh.shape['fsdp']
    n_ep = mesh.shape['ep']
    n_dev = n_fsdp * n_ep
    all_axes = ('fsdp', 'ep')
    tok_spec = P(('ep', 'fsdp'), None)
    up_spec = P('ep', 'fsdp', None)
    down_spec = P('ep', None, 'fsdp')

    def local_step(x_loc, dy_loc, ids_loc, slot_loc, w_router, wg_loc, wu_loc, wd_loc):
        tok_dev, _ = x_loc.shape
        top_k = ids_loc.shape[1]
        n_exp = w_router.shape[1]
        local_exp = n_exp // n_ep
        tokens = tok_dev * n_dev
        halves = tok_dev // BLK
        f_idx = lax.axis_index('fsdp')
        ep_idx = lax.axis_index('ep')
        bits = [(ep_idx // d) % 2 == 1 for d in (4, 2, 1)]

        loc = (wg_loc, wu_loc, wd_loc)
        n2 = local_exp // 2
        other_w = [[hop_z(w[p * n2:(p + 1) * n2]) for w in loc] for p in range(2)]

        xd = {(0, h): turn(jnp.stack([x_loc[h * BLK:(h + 1) * BLK], dy_loc[h * BLK:(h + 1) * BLK]]), f_idx) for h in range(2)}
        xd[X, 0] = hop(xd[0, 0], X)
        xd[Y, 1] = hop(xd[0, 1], Y)
        xd[X, 1] = hop(xd[0, 1], X)
        xd[Y, 0] = hop(xd[0, 0], Y)
        xd[X + Y, 1] = hop(xd[Y, 1], X)
        xd[X + Y, 0] = hop(xd[X, 0], Y)

        logits = dot(w_router, x_loc, 0, 1)
        prob = jax.nn.softmax(logits, axis=0)
        expert = jnp.arange(n_exp, dtype=jnp.int32)[None, :, None]
        match = ids_loc.T[:, None, :] == expert
        chosen = jnp.any(match, axis=0)
        kept = jnp.any(match & (slot_loc.T[:, None, :] >= 0), axis=0)
        stat = jnp.stack([jnp.sum(chosen.astype(F32), axis=1), jnp.sum(prob, axis=1)])

        upto = jnp.arange(BLK)[:, None] <= jnp.arange(BLK)[None, :]
        kept_b = kept.astype(BF16).reshape(n_exp * halves, BLK)
        place = dot(kept_b, upto.astype(BF16), 1, 0).reshape(n_exp, tok_dev) - 1.0
        pos = jnp.where(kept, place, -1.0)
        gate = jnp.where(kept, prob, 0.0)
        meta = jnp.stack([pos, gate], axis=1).reshape(n_ep, local_exp, 2, tok_dev)
        own_meta = lax.dynamic_index_in_dim(meta, ep_idx, 0, keepdims=False)
        peer_meta = hop(lax.dynamic_index_in_dim(meta, ep_idx ^ 1, 0, keepdims=False), 1)
        far_meta = lax.all_to_all(meta, 'ep', 0, 0, tiled=True)

        def blocked(m):
            m = m.reshape(-1, local_exp, 2, halves, BLK).transpose(3, 0, 1, 2, 4)
            nt = ((jnp.max(m[..., 0, :], axis=-1) + TILE // 2) / (TILE // 2)).astype(jnp.int32)
            return nt, m[..., 0:1, :], m[..., 1:2, :]

        metas = [blocked(jnp.stack([own_meta, peer_meta])), None]

        def meta_of(sets, e_lo, e_hi):
            out = []
            for j in range(3):
                rows = [metas[k != 0][j][h, k:k + 2, e_lo:e_hi] for k, h in sets]
                out.append(jnp.concatenate(rows, axis=0))
            return out

        own_sets = ((0, 0), (0, 1))
        near = ((X, 0), (Y, 1))
        diag = ((X + Y, 0), (X + Y, 1))
        last = ((Y, 0), (X, 1))
        calls = [(own_sets[:1], 0, 2), (own_sets[1:], 0, 2), (near, 0, 4), (diag, 0, 4), (last, 0, 2), (last, 2, 4), (own_sets, 2, 4)]
        acc = [None, None]
        part, dgate, raw = {}, {}, {}
        first_weights = [w for i, m in enumerate(loc) for w in (m, other_w[0][i])]

        def core_hop(k, h):
            xd[k + 1, h] = hop(xd[k, h], 1)

        for k, h in own_sets:
            core_hop(k, h)

        def reduce_core(n, sets):
            for k, h in sets:
                mine, theirs = raw[n, k, h]
                other = hop(theirs, 1)
                part[n, k, h] = [mine[i] + other[i] for i in range(2)]

        stat_bits = [1, X, Y]
        for n, (sets, e_lo, e_hi) in enumerate(calls):
            nt, pos_k, gate_k = meta_of(sets, e_lo, e_hi)
            if n in (3, 4):
                ready = calls[n - 1][0]
                nt, done = lax.optimization_barrier((nt, [part[n - 1, k, h] for k, h in ready]))
                for (k, h), d in zip(ready, done):
                    part[n - 1, k, h] = d
            toks = [xd[k + c, h] for k, h in sets for c in range(2)]
            pairs = slice(e_lo // 2, e_hi // 2)
            outs, dgate[n], acc[pairs] = experts(
                nt, pos_k, gate_k, toks, first_weights if n < 2 else weights, e_lo, acc[pairs])
            for j, (k, h) in enumerate(sets):
                raw[n, k, h] = outs[2 * j:2 * j + 2]
            if n not in (4, 5):
                reduce_core(n, sets)
            if n == 0:
                xd[X, 0], xd[Y, 1], dgate[n] = lax.optimization_barrier((xd[X, 0], xd[Y, 1], dgate[n]))
                for k, h in near:
                    core_hop(k, h)
            if n == 1:
                far_meta, other_w[1], dgate[n] = lax.optimization_barrier((far_meta, other_w[1], dgate[n]))
                metas[1] = blocked(by_distance(far_meta, bits))
                weights = [w for i, m in enumerate(loc) for w in (m, jnp.concatenate([other_w[0][i], other_w[1][i]], axis=0))]
            if n == 2:
                for k, h in diag + last:
                    xd[k, h], dgate[n] = lax.optimization_barrier((xd[k, h], dgate[n]))
                    core_hop(k, h)
            if n < 4:
                stat, dgate[n] = lax.optimization_barrier((stat, dgate[n]))
                stat = stat + (hop(stat, stat_bits[n]) if n < 3 else hop_z(stat))

        direct = [[hop(part[2, X, 0][i], X), hop(part[2, Y, 1][i], Y)] for i in range(2)]
        diagonal = [[hop(part[3, X + Y, 0][i], X), hop(part[3, X + Y, 1][i], Y)] for i in range(2)]
        ends = [[raw[n, k, h][0] for n in (4, 5)] + [hop(raw[n, k, h][1], 1) for n in (4, 5)] for k, h in last]
        relay = []
        for i in range(2):
            sums = [(m0[i] + o0[i]) + (m1[i] + o1[i]) + d for (m0, m1, o0, o1), d in zip(ends, diagonal[i])]
            ends, sums = lax.optimization_barrier((ends, sums))
            relay.append([hop(sums[0], Y), hop(sums[1], X)])

        grads = []
        for p in range(2):
            got = hop_z(acc[p][1])
            grads.append((acc[p][0] + got).astype(BF16))
        dwg, dwu, dwd = (jnp.concatenate([g[:, i] for g in grads], axis=0) for i in range(3))

        def dgate_of(n):
            d = dgate[n]
            return d.reshape(-1, 2, d.shape[1], BLK)

        far = {}
        for n, sets in ((2, near), (3, diag), (4, last), (5, last)):
            d = dgate_of(n)
            for j, (k, h) in enumerate(sets):
                for c in range(2):
                    far.setdefault((k + c, h), []).append(d[j, c])
        zero = jnp.zeros((local_exp, BLK), F32)
        far = jnp.stack([jnp.concatenate([jnp.concatenate(far.get((k, h), [zero]), axis=0) for h in range(halves)], axis=1) for k in range(n_ep)])
        far = by_distance(far, bits)
        far = lax.all_to_all(far, 'ep', 0, 0, tiled=True)
        own = jnp.concatenate([jnp.concatenate([dgate_of(0), dgate_of(1)], axis=0), dgate_of(6)], axis=2)
        own = own.transpose(1, 2, 0, 3).reshape(2, local_exp, tok_dev)
        peer = hop(own[1], 1)
        far = by_distance(far, bits)
        d_gate = by_distance(jnp.concatenate([own[:1], peer[None], far[2:]], axis=0), bits).reshape(n_exp, tok_dev)

        load_frac = stat[0] / (tokens * top_k)
        aux_loss = AUX_COEF * n_exp * jnp.sum(load_frac * stat[1] / tokens)
        d_prob = d_gate + AUX_COEF * n_exp * load_frac[:, None]
        d_logit = (prob * (d_prob - jnp.sum(prob * d_prob, axis=0, keepdims=True))).astype(BF16)
        dw_router = lax.psum(dot(x_loc, d_logit, 0, 1), all_axes)

        pre = [[part[h, 0, h][i] + part[6, 0, h][i] + direct[i][h] for h in range(2)] for i in range(2)]
        pre = lax.optimization_barrier(pre)
        y = turn(jnp.concatenate([pre[0][h] + relay[0][h] for h in range(2)], axis=0).astype(BF16), f_idx)
        y, pre = lax.optimization_barrier((y, pre))
        dx_exp = jnp.concatenate([pre[1][h] + relay[1][h] for h in range(2)], axis=0)
        dx = (turn(dx_exp, f_idx) + dot(d_logit, w_router, 0, 1)).astype(BF16)
        return y, aux_loss, dx, dw_router, dwg, dwu, dwd

    return jax.shard_map(local_step, mesh=mesh,
                         in_specs=(tok_spec, tok_spec, tok_spec, tok_spec, P(), up_spec, up_spec, down_spec),
                         out_specs=(tok_spec, P(), tok_spec, P(), up_spec, up_spec, down_spec),
                         check_vma=False)
```

```python
import functools

import jax
import jax.numpy as jnp
from jax import lax
from jax.experimental import pallas as pl
from jax.experimental.pallas import tpu as pltpu
from jax.sharding import PartitionSpec as P


AUX_COEF = 0.01
BLK = 1024
TILE = 256
NARROW = 256
X, Y = 2, 4
F32 = jnp.float32
BF16 = jnp.bfloat16


def dot(a, b, ca, cb):
    return lax.dot_general(a, b, (((ca,), (cb,)), ((), ())), preferred_element_type=F32)


def expert_kernel(n_blk, n_exp, fresh, nt_ref, win_ref, pos_ref, gate_ref, wg0_ref, wg1_ref, wu0_ref, wu1_ref, wd0_ref, wd1_ref, *rest):
    n_pair = n_exp // 2
    rest = list(rest)
    take = lambda n: [rest.pop(0) for _ in range(n)]
    tok_in_refs = take(n_blk)
    acc_in_refs = [None if fresh[p] else take(2) for p in range(n_pair)]
    tok_out_refs = take(n_blk)
    dgate_ref, = take(1)
    acc_out_refs = [take(2) for _ in range(n_pair)]
    xd_ref, yd_ref, acc_ref, in_sem, out_sem, acc_in_sem, acc_out_sem = rest
    b = pl.program_id(0)
    e = pl.program_id(1)
    half = xd_ref.shape[3] // 2
    tok_in = [pltpu.make_async_copy(src, xd_ref.at[k % 2], in_sem.at[k]) for k, src in enumerate(tok_in_refs)]
    tok_out = [pltpu.make_async_copy(yd_ref.at[k % 2], dst, out_sem.at[k]) for k, dst in enumerate(tok_out_refs)]

    def acc_in(k):
        return [pltpu.make_async_copy(acc_in_refs[k // 2][s].at[k % 2], acc_ref.at[k, s], acc_in_sem.at[k, s]) for s in range(2)]

    def acc_out(k):
        return [pltpu.make_async_copy(acc_ref.at[k, s], acc_out_refs[k // 2][s].at[k % 2], acc_out_sem.at[k, s]) for s in range(2)]

    @pl.when((b == 0) & (e == 0))
    def _():
        tok_in[0].start()
        if not fresh[0]:
            for c in acc_in(0):
                c.start()

    for k in range(n_exp):
        @pl.when((b == 0) & (e == k))
        def _():
            if k + 1 < n_exp and not fresh[(k + 1) // 2]:
                for c in acc_in(k + 1):
                    c.start()
            if k == n_exp // 2 - 1:
                tok_in[1].start()

    for k in range(n_blk):
        @pl.when((b == k) & (e == 0))
        def _():
            tok_in[k].wait()
            if 1 <= k < n_blk - 1:
                tok_in[k + 1].start()
            if k >= 2:
                tok_out[k - 2].wait()

    slot = b % 2

    @pl.when(e == 0)
    def _():
        yd_ref[slot] = jnp.zeros(yd_ref.shape[1:], F32)

    def acc_ready():
        for k in range(n_exp):
            @pl.when((b == 0) & (e == k))
            def _():
                if fresh[k // 2]:
                    acc_ref[k] = jnp.zeros(acc_ref.shape[1:], F32)
                else:
                    for c in acc_in(k):
                        c.wait()

    dgate_ref[...] = jnp.zeros(dgate_ref.shape, F32)
    wg, wu, wd = (wg0_ref, wg1_ref), (wu0_ref, wu1_ref), (wd0_ref, wd1_ref)
    cols = (slice(0, half), slice(half, 2 * half))

    def tile(base, size, first, tok, n_tok):
        pos = pos_ref[0, 0, :, tok]
        gate_row = gate_ref[0, 0, :, tok]
        rows = (lax.broadcasted_iota(jnp.int32, (size, n_tok), 0) + base).astype(F32)
        hit = rows == pos
        pick = jnp.where(hit, 1.0, 0.0).astype(BF16)
        gate_c = jnp.sum(jnp.where(hit, gate_row, 0.0), axis=1, keepdims=True)
        xc = [dot(pick, xd_ref[slot, 0, tok, c], 1, 0).astype(BF16) for c in cols]
        dyc = [dot(pick, xd_ref[slot, 1, tok, c], 1, 0) for c in cols]
        hg = dot(xc[0], wg[0][0], 1, 0) + dot(xc[1], wg[1][0], 1, 0)
        hu = dot(xc[0], wu[0][0], 1, 0) + dot(xc[1], wu[1][0], 1, 0)
        sig = jax.nn.sigmoid(hg)
        act = (hg * sig * hu).astype(BF16)
        do = [(gate_c * d).astype(BF16) for d in dyc]
        da = (dot(do[0], wd[0][0], 1, 1) + dot(do[1], wd[1][0], 1, 1)).astype(BF16).astype(F32)
        dhg = (da * hu * sig * (1.0 + hg * (1.0 - sig))).astype(BF16)
        dhu = (da * hg * sig).astype(BF16)
        o = [dot(act, w[0], 1, 0).astype(BF16) for w in wd]
        dgate_c = sum(jnp.sum(dyc[s] * o[s].astype(F32), axis=1, keepdims=True) for s in range(2))
        dgate_ref[0, 0, :, tok] += jnp.sum(jnp.where(hit, dgate_c, 0.0), axis=0, keepdims=True)
        db = [(dot(dhg, wg[s][0], 1, 1) + dot(dhu, wu[s][0], 1, 1)).astype(BF16) for s in range(2)]
        pl.when(first)(acc_ready)
        for s in range(2):
            acc_ref[e, s, 0] += dot(xc[s], dhg, 0, 0)
            acc_ref[e, s, 1] += dot(xc[s], dhu, 0, 0)
            acc_ref[e, s, 2] += dot(act, do[s], 0, 0)
        gate_t = jnp.transpose(jnp.broadcast_to(gate_row, (8, n_tok)))[:, :1]
        width = 256
        for s in range(2):
            for c in range(half // width):
                part = slice(c * width, (c + 1) * width)
                out = slice(s * half + c * width, s * half + (c + 1) * width)
                yd_ref[slot, 0, tok, out] += gate_t * dot(pick, o[s][:, part], 0, 0)
                yd_ref[slot, 1, tok, out] += dot(pick, db[s][:, part], 0, 0)

    every = pl.ds(0, BLK)

    def full_tile(i, carry):
        tile(i * TILE, TILE, i == 0, every, BLK)
        return carry

    tiles = nt_ref[b, e]
    start = win_ref[b, e]
    full = jnp.right_shift(tiles, 1)
    lax.fori_loop(0, full, full_tile, 0)
    rest_rows = (tiles & 1) == 1

    @pl.when(rest_rows & (start >= 0))
    def _():
        tok = pl.ds(pl.multiple_of(jnp.maximum(start, 0), 128), NARROW)
        tile(full * TILE, TILE // 2, full == 0, tok, NARROW)

    @pl.when(rest_rows & (start < 0))
    def _():
        tile(full * TILE, TILE // 2, full == 0, every, BLK)

    pl.when(tiles == 0)(acc_ready)

    for k in range(n_blk):
        @pl.when((b == k) & (e == n_exp - 1))
        def _():
            tok_out[k].start()

    for k in range(n_exp):
        @pl.when((b == n_blk - 1) & (e == k))
        def _():
            for c in acc_out(k):
                c.start()

    @pl.when((b == n_blk - 1) & (e == n_exp - 1))
    def _():
        for k in range(max(0, n_blk - 2), n_blk):
            tok_out[k].wait()
        for k in range(n_exp):
            for c in acc_out(k):
                c.wait()


def experts(nt, win, pos, gate, toks, weights, e0, acc):
    n_blk, n_exp = nt.shape
    d_model = toks[0].shape[2]
    half, d_ff = weights[0].shape[1:]
    row = pl.BlockSpec((1, 1, 1, BLK), lambda b, e, nt, win: (b, e, 0, 0))
    up = pl.BlockSpec((1, half, d_ff), lambda b, e, nt, win: (e + e0, 0, 0))
    down = pl.BlockSpec((1, d_ff, half), lambda b, e, nt, win: (e + e0, 0, 0))
    hbm = pl.BlockSpec(memory_space=pl.ANY)
    fresh = tuple(a is None for a in acc)
    acc_args = [r for a in acc if a is not None for r in a]
    acc_shape = jax.ShapeDtypeStruct((2, 3, half, d_ff), F32)
    first_in = 2 + 8 + n_blk
    first_out = n_blk + 1
    aliases = {}
    for p, a in enumerate(acc):
        if a is not None:
            for s in range(2):
                aliases[first_in] = first_out + 2 * p + s
                first_in += 1
    res = pl.pallas_call(
        functools.partial(expert_kernel, n_blk, n_exp, fresh),
        grid_spec=pltpu.PrefetchScalarGridSpec(
            num_scalar_prefetch=2,
            grid=(n_blk, n_exp),
            in_specs=[row, row, up, up, up, up, down, down] + [hbm] * (n_blk + len(acc_args)),
            out_specs=[hbm] * n_blk + [row] + [hbm] * (2 * len(acc)),
            scratch_shapes=[
                pltpu.VMEM((2, 2, BLK, d_model), BF16),
                pltpu.VMEM((2, 2, BLK, d_model), F32),
                pltpu.VMEM((n_exp, 2, 3, half, d_ff), F32),
                pltpu.SemaphoreType.DMA((n_blk,)),
                pltpu.SemaphoreType.DMA((n_blk,)),
                pltpu.SemaphoreType.DMA((n_exp, 2)),
                pltpu.SemaphoreType.DMA((n_exp, 2)),
            ],
        ),
        out_shape=[jax.ShapeDtypeStruct((2, BLK, d_model), F32)] * n_blk
        + [jax.ShapeDtypeStruct((n_blk, n_exp, 1, BLK), F32)] + [acc_shape] * (2 * len(acc)),
        input_output_aliases=aliases,
        compiler_params=pltpu.CompilerParams(
            dimension_semantics=("arbitrary", "arbitrary"), vmem_limit_bytes=67_000_000),
        cost_estimate=pl.CostEstimate(flops=100_000_000, bytes_accessed=80_000_000, transcendentals=1_000_000),
    )(nt, win, pos, gate, *weights, *toks, *acc_args)
    toks_out, dgate, acc = res[:n_blk], res[n_blk], res[n_blk + 1:]
    return toks_out, dgate, [acc[2 * p:2 * p + 2] for p in range(len(acc) // 2)]


def by_distance(a, bits):
    rest = a.shape[1:]
    a = a.reshape(2, 2, 2, *rest)
    for axis, bit in enumerate(bits):
        a = jnp.where(bit, jnp.flip(a, axis), a)
    return a.reshape(8, *rest)


def hop(a, bit):
    return lax.ppermute(a, 'ep', [(i, i ^ bit) for i in range(8)])


def hop_z(a):
    return lax.ppermute(a, 'fsdp', [(0, 1), (1, 0)])


def turn(a, f_idx):
    half = a.shape[-1] // 2
    return jnp.where(f_idx == 1, jnp.concatenate([a[..., half:], a[..., :half]], axis=-1), a)


def solution(mesh):
    n_fsdp = mesh.shape['fsdp']
    n_ep = mesh.shape['ep']
    n_dev = n_fsdp * n_ep
    all_axes = ('fsdp', 'ep')
    tok_spec = P(('ep', 'fsdp'), None)
    up_spec = P('ep', 'fsdp', None)
    down_spec = P('ep', None, 'fsdp')

    def local_step(x_loc, dy_loc, ids_loc, slot_loc, w_router, wg_loc, wu_loc, wd_loc):
        tok_dev, _ = x_loc.shape
        top_k = ids_loc.shape[1]
        n_exp = w_router.shape[1]
        local_exp = n_exp // n_ep
        tokens = tok_dev * n_dev
        halves = tok_dev // BLK
        f_idx = lax.axis_index('fsdp')
        ep_idx = lax.axis_index('ep')
        bits = [(ep_idx // d) % 2 == 1 for d in (4, 2, 1)]

        loc = (wg_loc, wu_loc, wd_loc)
        n2 = local_exp // 2
        other_w = [[hop_z(w[p * n2:(p + 1) * n2]) for w in loc] for p in range(2)]

        xd = {(0, h): turn(jnp.stack([x_loc[h * BLK:(h + 1) * BLK], dy_loc[h * BLK:(h + 1) * BLK]]), f_idx) for h in range(2)}
        xd[X, 0] = hop(xd[0, 0], X)
        xd[Y, 1] = hop(xd[0, 1], Y)
        xd[X, 1] = hop(xd[0, 1], X)
        xd[Y, 0] = hop(xd[0, 0], Y)
        xd[X + Y, 1] = hop(xd[Y, 1], X)
        xd[X + Y, 0] = hop(xd[X, 0], Y)

        logits = dot(w_router, x_loc, 0, 1)
        prob = jax.nn.softmax(logits, axis=0)
        expert = jnp.arange(n_exp, dtype=jnp.int32)[None, :, None]
        match = ids_loc.T[:, None, :] == expert
        chosen = jnp.any(match, axis=0)
        kept = jnp.any(match & (slot_loc.T[:, None, :] >= 0), axis=0)
        stat = jnp.stack([jnp.sum(chosen.astype(F32), axis=1), jnp.sum(prob, axis=1)])

        upto = jnp.arange(BLK)[:, None] <= jnp.arange(BLK)[None, :]
        kept_b = kept.astype(BF16).reshape(n_exp * halves, BLK)
        place = dot(kept_b, upto.astype(BF16), 1, 0).reshape(n_exp, tok_dev) - 1.0
        pos = jnp.where(kept, place, -1.0)
        gate = jnp.where(kept, prob, 0.0)
        meta = jnp.stack([pos, gate], axis=1).reshape(n_ep, local_exp, 2, tok_dev)
        own_meta = lax.dynamic_index_in_dim(meta, ep_idx, 0, keepdims=False)
        peer_meta = hop(lax.dynamic_index_in_dim(meta, ep_idx ^ 1, 0, keepdims=False), 1)
        far_meta = lax.all_to_all(meta, 'ep', 0, 0, tiled=True)

        def blocked(m):
            m = m.reshape(-1, local_exp, 2, halves, BLK).transpose(3, 0, 1, 2, 4)
            place = m[..., 0, :]
            nt = jnp.floor((jnp.max(place, axis=-1) + TILE // 2) / (TILE // 2))
            at = jnp.arange(BLK, dtype=jnp.int32)
            inside = place >= jnp.floor(nt / 2)[..., None] * TILE
            lo = jnp.min(jnp.where(inside, at, BLK), axis=-1)
            hi = jnp.max(jnp.where(inside, at, -1), axis=-1)
            start = jnp.minimum(lo // 128 * 128, BLK - NARROW)
            return nt.astype(jnp.int32), jnp.where(hi - start < NARROW, start, -1), m[..., 0:1, :], m[..., 1:2, :]

        metas = [blocked(jnp.stack([own_meta, peer_meta])), None]

        def meta_of(sets, e_lo, e_hi):
            out = []
            for j in range(4):
                rows = [metas[k != 0][j][h, k:k + 2, e_lo:e_hi] for k, h in sets]
                out.append(jnp.concatenate(rows, axis=0))
            return out

        own_sets = ((0, 0), (0, 1))
        near = ((X, 0), (Y, 1))
        diag = ((X + Y, 0), (X + Y, 1))
        last = ((Y, 0), (X, 1))
        calls = [(own_sets[:1], 0, 2), (own_sets[1:], 0, 2), (near, 0, 4), (diag, 0, 4), (last, 0, 2), (last, 2, 4), (own_sets, 2, 4)]
        acc = [None, None]
        part, dgate, raw = {}, {}, {}
        first_weights = [w for i, m in enumerate(loc) for w in (m, other_w[0][i])]

        def core_hop(k, h):
            xd[k + 1, h] = hop(xd[k, h], 1)

        for k, h in own_sets:
            core_hop(k, h)

        def reduce_core(n, sets):
            for k, h in sets:
                mine, theirs = raw[n, k, h]
                other = hop(theirs, 1)
                part[n, k, h] = [mine[i] + other[i] for i in range(2)]

        stat_bits = [1, X, Y]
        for n, (sets, e_lo, e_hi) in enumerate(calls):
            nt, win, pos_k, gate_k = meta_of(sets, e_lo, e_hi)
            if n in (3, 4):
                ready = calls[n - 1][0]
                nt, done = lax.optimization_barrier((nt, [part[n - 1, k, h] for k, h in ready]))
                for (k, h), d in zip(ready, done):
                    part[n - 1, k, h] = d
            toks = [xd[k + c, h] for k, h in sets for c in range(2)]
            pairs = slice(e_lo // 2, e_hi // 2)
            outs, dgate[n], acc[pairs] = experts(
                nt, win, pos_k, gate_k, toks, first_weights if n < 2 else weights, e_lo, acc[pairs])
            for j, (k, h) in enumerate(sets):
                raw[n, k, h] = outs[2 * j:2 * j + 2]
            if n not in (4, 5):
                reduce_core(n, sets)
            if n == 0:
                xd[X, 0], xd[Y, 1], dgate[n] = lax.optimization_barrier((xd[X, 0], xd[Y, 1], dgate[n]))
                for k, h in near:
                    core_hop(k, h)
            if n == 1:
                far_meta, other_w[1], dgate[n] = lax.optimization_barrier((far_meta, other_w[1], dgate[n]))
                metas[1] = blocked(by_distance(far_meta, bits))
                weights = [w for i, m in enumerate(loc) for w in (m, jnp.concatenate([other_w[0][i], other_w[1][i]], axis=0))]
            if n == 2:
                for k, h in diag + last:
                    xd[k, h], dgate[n] = lax.optimization_barrier((xd[k, h], dgate[n]))
                    core_hop(k, h)
            if n < 4:
                stat, dgate[n] = lax.optimization_barrier((stat, dgate[n]))
                stat = stat + (hop(stat, stat_bits[n]) if n < 3 else hop_z(stat))

        direct = [[hop(part[2, X, 0][i], X), hop(part[2, Y, 1][i], Y)] for i in range(2)]
        diagonal = [[hop(part[3, X + Y, 0][i], X), hop(part[3, X + Y, 1][i], Y)] for i in range(2)]
        ends = [[raw[n, k, h][0] for n in (4, 5)] + [hop(raw[n, k, h][1], 1) for n in (4, 5)] for k, h in last]
        relay = []
        for i in range(2):
            sums = [(m0[i] + o0[i]) + (m1[i] + o1[i]) + d for (m0, m1, o0, o1), d in zip(ends, diagonal[i])]
            ends, sums = lax.optimization_barrier((ends, sums))
            relay.append([hop(sums[0], Y), hop(sums[1], X)])

        grads = []
        for p in range(2):
            got = hop_z(acc[p][1])
            grads.append((acc[p][0] + got).astype(BF16))
        dwg, dwu, dwd = (jnp.concatenate([g[:, i] for g in grads], axis=0) for i in range(3))

        def dgate_of(n):
            d = dgate[n]
            return d.reshape(-1, 2, d.shape[1], BLK)

        far = {}
        for n, sets in ((2, near), (3, diag), (4, last), (5, last)):
            d = dgate_of(n)
            for j, (k, h) in enumerate(sets):
                for c in range(2):
                    far.setdefault((k + c, h), []).append(d[j, c])
        zero = jnp.zeros((local_exp, BLK), F32)
        far = jnp.stack([jnp.concatenate([jnp.concatenate(far.get((k, h), [zero]), axis=0) for h in range(halves)], axis=1) for k in range(n_ep)])
        far = by_distance(far, bits)
        far = lax.all_to_all(far, 'ep', 0, 0, tiled=True)
        own = jnp.concatenate([jnp.concatenate([dgate_of(0), dgate_of(1)], axis=0), dgate_of(6)], axis=2)
        own = own.transpose(1, 2, 0, 3).reshape(2, local_exp, tok_dev)
        peer = hop(own[1], 1)
        far = by_distance(far, bits)
        d_gate = by_distance(jnp.concatenate([own[:1], peer[None], far[2:]], axis=0), bits).reshape(n_exp, tok_dev)

        load_frac = stat[0] / (tokens * top_k)
        aux_loss = AUX_COEF * n_exp * jnp.sum(load_frac * stat[1] / tokens)
        d_prob = d_gate + AUX_COEF * n_exp * load_frac[:, None]
        d_logit = (prob * (d_prob - jnp.sum(prob * d_prob, axis=0, keepdims=True))).astype(BF16)
        dw_router = lax.psum(dot(x_loc, d_logit, 0, 1), all_axes)

        pre = [[part[h, 0, h][i] + part[6, 0, h][i] + direct[i][h] for h in range(2)] for i in range(2)]
        pre = lax.optimization_barrier(pre)
        y = turn(jnp.concatenate([pre[0][h] + relay[0][h] for h in range(2)], axis=0).astype(BF16), f_idx)
        y, pre = lax.optimization_barrier((y, pre))
        dx_exp = jnp.concatenate([pre[1][h] + relay[1][h] for h in range(2)], axis=0)
        dx = (turn(dx_exp, f_idx) + dot(d_logit, w_router, 0, 1)).astype(BF16)
        return y, aux_loss, dx, dw_router, dwg, dwu, dwd

    return jax.shard_map(local_step, mesh=mesh,
                         in_specs=(tok_spec, tok_spec, tok_spec, tok_spec, P(), up_spec, up_spec, down_spec),
                         out_specs=(tok_spec, P(), tok_spec, P(), up_spec, up_spec, down_spec),
                         check_vma=False)
```
